256 devices in a mesh: section: 2 (over y_hi), pb: 16 (over z, core), fsdp: 8 (over x, y_lo).
Axes of the slice: x: 4, y: 4 (y_hi: 2, y_lo: 2; y = y_hi * 2 + y_lo), z: 8, core: 2. Of those that a mesh axis runs over, the one named last changes fastest.
Arguments:
- decoder_states: bfloat16 [16, 32, 4096], P('pb', None, 'fsdp'), may hold values from -90 to 90
- norm_gain: bfloat16 [4096], P('fsdp'), may hold values from 0.099609375 to 1.8984375
- query_weight: bfloat16 [4096, 2048], P('fsdp', 'section'), may hold values from -0.046875 to 0.046875
- key_weight: bfloat16 [4096, 2048], P(('pb', 'fsdp'), 'section'), may hold values from -0.09375 to 0.09375
- value_weight: bfloat16 [4096, 2048], P(('pb', 'fsdp'), 'section'), may hold values from -0.09375 to 0.09375
- out_weight: bfloat16 [2048, 4096], P('section', 'fsdp'), may hold values from -0.5 to 0.5
- passage_states: bfloat16 [16, 4096, 4096], P('fsdp', 'pb'), may hold values from -400 to 400
- block_mask: int32 [16, 32], replicated, may hold values from 0 to 1, as said below
Outputs:
- cross_out: bfloat16 [16, 32, 4096], P('pb', None, 'fsdp')
The draws below stay inside these ranges and needn't reach their ends.
Inputs may be any that keep to these rules, and one draw needn't show every extreme that they name: `block_mask`: every question has at least one live block.
All inputs are finite; a program needn't handle non-finite values.
Results may differ from the reference program's by a relative error of at most 0.01.
The reference program's roundings to bfloat16 on the way (of `scaled`, `query`, `keys`, `values`, `weights` and `attention`) count: a program that leaves them out, or rounds other values in their place, can miss the bound.
Values may be sent and summed in bfloat16 or wider, within the bound.
A program may use at most 128 MiB of HBM per device.

```python
import jax
import jax.numpy as jnp
from jax import lax

D = 4096
HD = 64
HEADS = 32
ANSWER = 32
BLOCK = 128
INNER = 2048
QUESTIONS = 16
ROWS = 4096
BLOCKS = 32


def draw_decoder_states(key, part):
    base = jnp.clip(jax.random.normal(jax.random.fold_in(key, 1), (QUESTIONS, ANSWER, D), jnp.float32), -5.0, 5.0)
    column = 0.5 + jnp.arange(D, dtype=jnp.float32) / D
    return (base * column[None, None, :]).astype(jnp.bfloat16)


def draw_passage_states(key, part):
    base = jnp.clip(jax.random.normal(jax.random.fold_in(key, 4), (QUESTIONS, ROWS, D), jnp.float32), -5.0, 5.0)
    return base.astype(jnp.bfloat16)


def draw_block_mask(key, part):
    level = jax.random.randint(jax.random.fold_in(key, 11), (QUESTIONS, 1), 1, 9)
    ticket = jax.random.randint(jax.random.fold_in(key, 12), (QUESTIONS, BLOCKS), 0, 8)
    forced = jax.random.randint(jax.random.fold_in(key, 13), (QUESTIONS, 1), 0, BLOCKS)
    places = jnp.arange(BLOCKS, dtype=jnp.int32)[None, :]
    live_flags = (ticket < level) | (places == forced)
    return live_flags.astype(jnp.int32)


def level_of(stream_key, dims, shards, smallest, high):
    factor_of, own = 1.0, jax.random.fold_in(stream_key, 6)
    for axis_at, parts in shards:
        draws = jnp.exp(jax.random.uniform(jax.random.fold_in(own, axis_at), (parts,), jnp.float32, smallest / len(shards), high / len(shards)))
        factor_of = factor_of * jnp.repeat(draws, dims[axis_at] // parts).reshape([-1 if axis == axis_at else 1 for axis in range(len(dims))])
    return factor_of


def centred(key, shape, spread, most, split=(), kind=jnp.bfloat16):
    drawn = spread * jax.random.normal(key, shape, jnp.float32)
    if split:
        drawn = drawn * level_of(key, shape, split, -0.22, 0.18)
    return jnp.clip(drawn, -most, most).astype(kind)


def setup_inputs(seed: int = 0) -> dict:
    key_list = jax.random.split(jax.random.key(seed), 9)
    return {
        "decoder_states": draw_decoder_states(jax.random.fold_in(key_list[8], 71), 0),
        "norm_gain": jnp.clip(1.0 + 0.18 * jax.random.normal(key_list[1], (D,), jnp.float32), 0.099609375, 1.8984375).astype(jnp.bfloat16),
        "query_weight": centred(key_list[2], (D, INNER), (4 * D) ** -0.5, 0.046875, ((0, 8), (1, 2))),
        "key_weight": centred(key_list[3], (D, INNER), D ** -0.5, 0.09375, ((0, 128), (1, 2))),
        "value_weight": centred(key_list[4], (D, INNER), D ** -0.5, 0.09375, ((0, 128), (1, 2))),
        "out_weight": centred(key_list[5], (INNER, D), (INNER // 16) ** -0.5, 0.5, ((0, 2), (1, 8))),
        "passage_states": draw_passage_states(jax.random.fold_in(key_list[8], 71), 0),
        "block_mask": draw_block_mask(jax.random.fold_in(key_list[8], 71), 0),
    }


NEGATIVE = -1e+30

def rounded(value):
    return lax.optimization_barrier(value.astype(jnp.bfloat16))

def reference(decoder_states, norm_gain, query_weight, key_weight, value_weight, out_weight, passage_states, block_mask):
    states_wide = decoder_states.astype(jnp.float32)
    square_mean = lax.optimization_barrier(jnp.mean(states_wide * states_wide, axis=2))
    scaled = rounded(states_wide * norm_gain.astype(jnp.float32)[None, None, :])
    query_raw = jnp.einsum('qad,de->qae', scaled.astype(jnp.float32), query_weight.astype(jnp.float32))
    query = (query_raw * lax.rsqrt(square_mean + 1e-06)[:, :, None]).astype(jnp.bfloat16)
    row_live = jnp.repeat(block_mask, BLOCK, axis=1) > 0

    def one_question(packed):
        passages, question, visible = packed
        keys = rounded(jnp.dot(passages, key_weight, preferred_element_type=jnp.float32))
        values = rounded(jnp.dot(passages, value_weight, preferred_element_type=jnp.float32))
        queries = question.reshape(ANSWER, HEADS, HD).astype(jnp.float32)
        keys_split = keys.reshape(ROWS, HEADS, HD).astype(jnp.float32)
        values_split = values.reshape(ROWS, HEADS, HD).astype(jnp.float32)
        scores = jnp.einsum('ahd,rhd->ahr', queries, keys_split)
        shown = visible[None, None, :]
        scores = jnp.where(shown, scores, NEGATIVE)
        peak = lax.optimization_barrier(jnp.max(scores, axis=2, keepdims=True))
        raw_weights = jnp.where(shown, jnp.exp(scores - peak), 0.0)
        totals = lax.optimization_barrier(jnp.sum(raw_weights, axis=2, keepdims=True))
        weights = rounded(raw_weights)
        numerator = jnp.einsum('ahr,rhd->ahd', weights.astype(jnp.float32), values_split)
        attention = (numerator / totals).astype(jnp.bfloat16).reshape(ANSWER, INNER)
        return jnp.dot(attention, out_weight, preferred_element_type=jnp.float32).astype(jnp.bfloat16)
    return lax.map(one_question, (passage_states, query, row_live))
```

```python
import jax
import jax.numpy as jnp
from jax import lax
from jax.experimental import pallas as pl
from jax.experimental.pallas import tpu as pltpu
from jax.sharding import PartitionSpec as P

HD = 64
BLOCK = 128
NEGATIVE = -1e30
MESH = pl.DeviceIdType.MESH
NZ = 8
NX = 4
SPLIT = 384
F32 = jnp.float32
BF16 = jnp.bfloat16


def kernel(
    mask_ref, ds_ref, gain_ref, qw_ref, kw_ref, vw_ref, ow_ref, pass_ref, out_ref,
    xs, ws, acc, ow, ds, gain, qw, qpart, qrecv, qsend, qbuf, part, recv, asend, att,
    loc, pair_s, pair_r, y_s, y_r, ax_s, ax_r, az_s, az_r, bz_s, bz_r, bx_s, bx_r,
    q2_s, q2_r, q3_s, q3_r, ow_s, ow_r, t1_s, t1_r, t2_s, t2_r,
):
    s = lax.axis_index("section")
    p = lax.axis_index("pb")
    f = lax.axis_index("fsdp")
    z, c = p // 2, lax.rem(p, 2)
    x, y = f // 2, lax.rem(f, 2)

    def zat(k):
        return lax.rem(z + k + NZ, NZ)

    def xat(k):
        return lax.rem(x + k + NX, NX)

    def dev(s_, p_, f_):
        return {"section": s_, "pb": p_, "fsdp": f_}

    partner = dev(s, z * 2 + 1 - c, f)
    ynear = dev(s, p, x * 2 + 1 - y)
    xdev = {k: dev(s, p, xat(k) * 2 + y) for k in (1, -1)}
    zdev = {k: dev(s, zat(k) * 2 + c, f) for k in (1, -1)}
    other_section = dev(1 - s, p, f)

    def rcopy(src, dst, ssem, rsem, to):
        return pltpu.make_async_remote_copy(
            src_ref=src, dst_ref=dst, send_sem=ssem, recv_sem=rsem, device_id=to, device_id_type=MESH
        )

    def half(ref, h):
        return ref.at[:, pl.ds(pl.multiple_of(h * 512, 512), 512)]

    locals_ = [
        pltpu.make_async_copy(ds_ref, ds, loc.at[0]),
        pltpu.make_async_copy(gain_ref, gain, loc.at[1]),
        pltpu.make_async_copy(qw_ref, qw, loc.at[2]),
        pltpu.make_async_copy(half(kw_ref, c), ws.at[z, c, f, :, pl.ds(0, 512)], loc.at[3]),
        pltpu.make_async_copy(half(vw_ref, c), ws.at[z, c, f, :, pl.ds(512, 512)], loc.at[4]),
        pltpu.make_async_copy(pass_ref, xs.at[c], loc.at[5]),
        pltpu.make_async_copy(ow_ref, ow.at[s], loc.at[6]),
    ]
    for copy in locals_:
        copy.start()

    barrier = pltpu.get_barrier_semaphore()

    def greet(to):
        pl.semaphore_signal(barrier, inc=1, device_id=to, device_id_type=MESH)

    def greet_maybe(is_self, to):
        @pl.when(jnp.logical_not(is_self))
        def _():
            greet(to)

    def q3_target(k):
        return zat(k), f // 4, z

    def t2_target(ds_, k):
        return lax.rem(s + ds_, 2), f * 2 + z // 4, lax.rem(f + k, 8)

    for to in (partner, ynear, xdev[1], xdev[-1], zdev[1], zdev[-1], other_section):
        greet(to)
    for k in range(1, 8):
        greet(dev(s, p, lax.rem(f + k, 8)))
        greet(dev(s, zat(k) * 2 + c, f))
    diag = z == f
    for k in range(8):
        zt, ct, ft = q3_target(k)
        to = dev(s, zt * 2 + ct, ft)
        if k == 0:
            greet_maybe(diag & (ct == c), to)
        else:
            greet(to)
    for ds_ in range(2):
        for k in range(8):
            st, pt, ft = t2_target(ds_, k)
            to = dev(st, pt, ft)
            if ds_ == 0 and k == 0:
                greet_maybe(pt == p, to)
            else:
                greet(to)
    selves = jnp.where(diag & (f // 4 == c), 1, 0) + jnp.where(f * 2 + z // 4 == p, 1, 0)
    pl.semaphore_wait(barrier, 7 + 14 + 8 + 16 - selves)

    sends = []

    def go(copy):
        copy.start()
        sends.append(copy)

    def pair_copy(i):
        w_ref = (kw_ref, vw_ref)[i]
        return rcopy(
            half(w_ref, 1 - c), ws.at[z, c, f, :, pl.ds(512 * i, 512)], pair_s.at[i], pair_r.at[i], partner
        )

    go(pair_copy(0))
    go(pair_copy(1))
    go(rcopy(pass_ref, xs.at[c], pair_s.at[2], pair_r.at[2], partner))

    def land(dst, rsem):
        rcopy(dst, dst, loc.at[7], rsem, partner).wait_recv()

    def plane(i):
        if i == 0:
            return z
        if i == NZ - 1:
            return zat(NZ // 2)
        return zat(-((i + 1) // 2)) if i % 2 else zat(i // 2)

    def piece_a(zz, xx):
        return ws.at[zz, :, pl.ds(xx * 2, 2), :, pl.ds(0, SPLIT)]

    def piece_b(zz, xx):
        return ws.at[zz, :, pl.ds(xx * 2, 2), :, pl.ds(SPLIT, 1024 - SPLIT)]

    def piece_bh(zz, xx, h):
        return ws.at[zz, h, pl.ds(xx * 2, 2), :, pl.ds(SPLIT, 1024 - SPLIT)]

    def onward(i, parity):
        if i == NZ - 1:
            return None
        k = (i + 1) // 2
        way = 1 if i % 2 else -1
        if k + 1 < NZ // 2:
            return (i + 2, way)
        if (parity == 0) == (way == 1):
            return (NZ - 1, way)
        return None

    def z_sends(ref, i, col, ssem, rsem):
        nexts = [(1, 1), (2, -1)] if i == 0 else [onward(i, col % 2)]
        for step in nexts:
            if step is not None:
                slot, way = step
                go(rcopy(ref, ref, ssem.at[slot - 1, col], rsem.at[slot - 1, col], zdev[way]))

    xorder = (0, -1, 1, 2)

    def b_z(i):
        for h in range(2):
            ref = piece_bh(plane(i), x, h)
            if i > 0:
                land(ref, bz_r.at[i - 1, h])
            z_sends(ref, i, h, bz_s, bz_r)
        ref = piece_b(plane(i), x)
        go(rcopy(ref, ref, bx_s.at[i, 0], bx_r.at[i, 0], xdev[1]))
        go(rcopy(ref, ref, bx_s.at[i, 1], bx_r.at[i, 1], xdev[-1]))

    def a_z(i):
        for j in range(4):
            ref = piece_a(plane(i), xat(xorder[j]))
            if i > 0:
                land(ref, az_r.at[i - 1, j])
            elif j > 0:
                land(ref, ax_r.at[j - 1])
                if j == 1:
                    go(rcopy(ref, ref, ax_s.at[2], ax_r.at[2], xdev[1]))
            z_sends(ref, i, j, az_s, az_r)

    def b_x1(i):
        left, right = piece_b(plane(i), xat(-1)), piece_b(plane(i), xat(1))
        land(left, bx_r.at[i, 0])
        if i % 2 == 0:
            go(rcopy(left, left, bx_s.at[i, 2], bx_r.at[i, 2], xdev[1]))
        land(right, bx_r.at[i, 1])
        if i % 2 == 1:
            go(rcopy(right, right, bx_s.at[i, 2], bx_r.at[i, 2], xdev[-1]))

    def b_x2(i):
        land(piece_b(plane(i), xat(2)), bx_r.at[i, 2])

    def project(i):
        zz = plane(i)
        cols = pl.ds(pl.multiple_of(zz * 512, 512), 512)

        def tile(t, carry):
            rows = xs[t // 2, lax.rem(t, 2), :, cols]
            for n in range(4):
                w = ws[zz, :, :, :, n * 256 : (n + 1) * 256].reshape(512, 256)
                term = jnp.dot(rows, w, preferred_element_type=F32)
                at = (t, slice(None), slice(n * 256, (n + 1) * 256))
                if i == 0:
                    acc[at] = term
                else:
                    acc[at] += term
            return carry

        lax.fori_loop(0, 4, tile, 0)

    def query_start():
        for copy in locals_[:3]:
            copy.wait()
        wide = ds[...].astype(F32)
        squares = jnp.broadcast_to(jnp.sum(wide * wide, axis=1, keepdims=True), (32, 128))
        scaled = (wide * gain[...].astype(F32)).astype(BF16)
        total = jnp.dot(scaled, qw[...], preferred_element_type=F32)
        for b in range(8):
            qpart[b, :, 0:128] = total[:, b * 128 : (b + 1) * 128]
            qpart[b, :, 128:256] = squares

    def query_reduce():
        for k in range(1, 8):
            to = lax.rem(f + k, 8)
            go(rcopy(qpart.at[to], qrecv.at[k - 1], q2_s.at[k - 1], q2_r.at[k - 1], dev(s, p, to)))

    def query_send():
        total = qpart[f]
        for k in range(7):
            land(qrecv.at[k], q2_r.at[k])
            total = total + qrecv[k]
        scale = lax.rsqrt(total[:, 128:256] / 4096.0 + 1e-06)
        qsend[...] = (total[:, 0:128] * scale).astype(BF16)
        block = lax.rem(f, 4)
        for k in range(8):
            zt, ct, ft = q3_target(k)
            copy = rcopy(
                qsend, qbuf.at[c, block], q3_s.at[k], q3_r.at[c * 4 + block], dev(s, zt * 2 + ct, ft)
            )
            if k == 0:
                own = diag & (ct == c)

                @pl.when(own)
                def _():
                    qbuf[c, block] = qsend[...]

                @pl.when(jnp.logical_not(own))
                def _():
                    copy.start()

            else:
                go(copy)

    def query_wait():
        for cs in range(2):
            for b in range(4):
                own = diag & (f // 4 == c) & (cs == c) & (b == lax.rem(f, 4))

                @pl.when(jnp.logical_not(own))
                def _():
                    land(qbuf.at[cs, b], q3_r.at[cs * 4 + b])

        zt, ct, ft = q3_target(0)

        @pl.when(jnp.logical_not(diag & (ct == c)))
        def _():
            rcopy(qsend, qbuf.at[0, 0], q3_s.at[0], q3_r.at[0], partner).wait_send()

    def attend():
        head_of = lax.broadcasted_iota(jnp.int32, (32, 512), 1) // HD
        lane = lax.broadcasted_iota(jnp.int32, (32, 128), 1)
        block_of = lax.broadcasted_iota(jnp.int32, (256, 512), 1) // BLOCK
        for q in range(2):
            query = jnp.concatenate([qbuf[q, b] for b in range(4)], axis=1).astype(F32)
            spread = jnp.concatenate(
                [jnp.where(head_of == h, query, 0.0).astype(BF16) for h in range(8)], axis=0
            )
            keys = jnp.concatenate([acc[q, :, 0:512], acc[2 + q, :, 0:512]], axis=0).astype(BF16)
            values = jnp.concatenate([acc[q, :, 512:1024], acc[2 + q, :, 512:1024]], axis=0).astype(BF16)
            scores = lax.dot_general(spread, keys, (((1,), (1,)), ((), ())), preferred_element_type=F32)
            flags = jnp.zeros((256, 512), jnp.int32)
            for b in range(4):
                flags = jnp.where(block_of == b, mask_ref[f * 2 + q, z * 4 + b], flags)
            shown = flags > 0
            scores = jnp.where(shown, scores, NEGATIVE)
            peak = jnp.max(scores, axis=1, keepdims=True)
            raw = jnp.where(shown, jnp.exp(scores - peak), 0.0)
            totals = jnp.sum(raw, axis=1, keepdims=True)
            wide = jnp.dot(raw.astype(BF16), values, preferred_element_type=F32)
            numer = jnp.zeros((32, 512), F32)
            stats = jnp.zeros((32, 128), F32)
            for h in range(8):
                rows = slice(h * 32, (h + 1) * 32)
                numer = jnp.where(head_of == h, wide[rows], numer)
                stats = jnp.where(lane == h, peak[rows], stats)
                stats = jnp.where(lane == h + 64, totals[rows], stats)
            for ah in range(2):
                rows = slice(ah * 16, (ah + 1) * 16)
                for ch in range(2):
                    rank = (q * 2 + ah) * 2 + ch
                    part[rank, :, 0:256] = numer[rows, ch * 256 : (ch + 1) * 256]
                    part[rank, :, 256:384] = stats[rows]

    def combine_send():
        for k in range(1, 8):
            zt = zat(k)
            go(rcopy(part.at[zt], recv.at[k - 1], t1_s.at[k - 1], t1_r.at[k - 1], dev(s, zt * 2 + c, f)))

    def combine():
        pieces = [part[z]]
        for k in range(7):
            land(recv.at[k], t1_r.at[k])
            pieces.append(recv[k])
        top = pieces[0][:, 256:384]
        for piece in pieces[1:]:
            top = jnp.maximum(top, piece[:, 256:384])
        col_head = lax.broadcasted_iota(jnp.int32, (16, 256), 1) // HD
        first = lax.rem(z, 2) == 0

        def widen(stat, base):
            low = jnp.zeros((16, 256), F32)
            for h in range(4):
                one = jnp.where(first, stat[:, base + h : base + h + 1], stat[:, base + h + 4 : base + h + 5])
                low = jnp.where(col_head == h, one, low)
            return low

        top_wide = widen(top, 0)
        numer = jnp.zeros((16, 256), F32)
        total = jnp.zeros((16, 256), F32)
        for piece in pieces:
            stat = piece[:, 256:384]
            factor = jnp.exp(widen(stat, 0) - top_wide)
            numer = numer + piece[:, 0:256] * factor
            total = total + widen(stat, 64) * factor
        asend[...] = (numer / total).astype(BF16)

    def spot():
        return s, c, lax.rem(z, 2), lax.rem(z // 2, 2)

    def scatter():
        a, b, d, e = spot()
        sem = t2_r.at[((a * 2 + b) * 2 + d) * 2 + e]
        for ds_ in range(2):
            for k in range(8):
                st, pt, ft = t2_target(ds_, k)
                copy = rcopy(asend, att.at[a, b, d, e], t2_s.at[ds_ * 8 + k], sem, dev(st, pt, ft))
                if ds_ == 0 and k == 0:
                    own = pt == p

                    @pl.when(own)
                    def _():
                        att[a, b, d, e] = asend[...]

                    @pl.when(jnp.logical_not(own))
                    def _():
                        copy.start()

                else:
                    go(copy)

    def finish():
        locals_[6].wait()
        land(ow.at[1 - s], ow_r.at[0])
        a, b, d, e = spot()
        own_code = ((a * 2 + b) * 2 + d) * 2 + e
        st, pt, ft = t2_target(0, 0)
        own = pt == p
        total = jnp.zeros((32, 512), F32)
        for si in range(2):
            for ci in range(2):
                for ch in range(2):
                    halves = []
                    for ah in range(2):
                        code = ((si * 2 + ci) * 2 + ch) * 2 + ah

                        @pl.when(jnp.logical_not(own & (own_code == code)))
                        def _():
                            land(att.at[si, ci, ch, ah], t2_r.at[code])

                        halves.append(att[si, ci, ch, ah])
                    rows = jnp.concatenate(halves, axis=0)
                    at = ci * 512 + ch * 256
                    total = total + jnp.dot(rows, ow[si, at : at + 256, :], preferred_element_type=F32)
        out_ref[...] = total.astype(BF16)

        @pl.when(jnp.logical_not(own))
        def _():
            rcopy(asend, att.at[0, 0, 0, 0], t2_s.at[0], t2_r.at[0], partner).wait_send()

    query_start()
    locals_[3].wait()
    locals_[4].wait()
    land(ws.at[z, 1 - c, f, :, pl.ds(0, 512)], pair_r.at[0])
    land(ws.at[z, 1 - c, f, :, pl.ds(512, 512)], pair_r.at[1])
    mine = ws.at[z, :, f]
    go(rcopy(mine, mine, y_s.at[0], y_r.at[0], ynear))
    land(ws.at[z, :, x * 2 + 1 - y], y_r.at[0])
    own_a = piece_a(z, x)
    go(rcopy(own_a, own_a, ax_s.at[0], ax_r.at[0], xdev[1]))
    go(rcopy(own_a, own_a, ax_s.at[1], ax_r.at[1], xdev[-1]))
    for t in range(NZ + 2):
        if t < NZ:
            b_z(t)
            a_z(t)
        if 1 <= t <= NZ:
            b_x1(t - 1)
        if t == 0:
            query_reduce()
        if t == 1:
            query_send()
        if t == 2:
            locals_[5].wait()
            land(xs.at[1 - c], pair_r.at[2])
            go(rcopy(ow_ref, ow.at[s], ow_s.at[0], ow_r.at[0], other_section))
        if t >= 2:
            b_x2(t - 2)
            project(t - 2)
    query_wait()
    attend()
    combine_send()
    combine()
    scatter()
    finish()
    for copy in sends:
        copy.wait_send()


def shards(
    decoder_states, norm_gain, query_weight, key_weight, value_weight, out_weight, passage_states, block_mask
):
    anywhere = pl.BlockSpec(memory_space=pl.ANY)
    dma = pltpu.SemaphoreType.DMA
    out = pl.pallas_call(
        kernel,
        out_shape=jax.ShapeDtypeStruct((32, 512), BF16),
        in_specs=[pl.BlockSpec(memory_space=pltpu.SMEM)] + [anywhere] * 7,
        out_specs=pl.BlockSpec(memory_space=pltpu.VMEM),
        scratch_shapes=[
            pltpu.VMEM((2, 2, 256, 4096), BF16),
            pltpu.VMEM((NZ, 2, 8, 32, 1024), BF16),
            pltpu.VMEM((4, 256, 1024), F32),
            pltpu.VMEM((2, 1024, 512), BF16),
            pltpu.VMEM((32, 512), BF16),
            pltpu.VMEM((1, 512), BF16),
            pltpu.VMEM((512, 1024), BF16),
            pltpu.VMEM((8, 32, 256), F32),
            pltpu.VMEM((7, 32, 256), F32),
            pltpu.VMEM((32, 128), BF16),
            pltpu.VMEM((2, 4, 32, 128), BF16),
            pltpu.VMEM((8, 16, 384), F32),
            pltpu.VMEM((7, 16, 384), F32),
            pltpu.VMEM((16, 256), BF16),
            pltpu.VMEM((2, 2, 2, 2, 16, 256), BF16),
            dma((8,)),
            dma((3,)), dma((3,)),
            dma((1,)), dma((1,)),
            dma((3,)), dma((3,)),
            dma((NZ - 1, 4)), dma((NZ - 1, 4)),
            dma((NZ - 1, 2)), dma((NZ - 1, 2)),
            dma((NZ, 3)), dma((NZ, 3)),
            dma((7,)), dma((7,)),
            dma((8,)), dma((8,)),
            dma((1,)), dma((1,)),
            dma((7,)), dma((7,)),
            dma((16,)), dma((16,)),
        ],
        compiler_params=pltpu.CompilerParams(
            collective_id=0, has_side_effects=True, vmem_limit_bytes=56 * 1024 * 1024
        ),
        name="reader",
    )(
        block_mask, decoder_states[0], norm_gain[None], query_weight, key_weight, value_weight,
        out_weight, passage_states,
    )
    return out[None]


def solution(mesh):
    placed = (
        P("pb", None, "fsdp"),
        P("fsdp"),
        P("fsdp", "section"),
        P(("pb", "fsdp"), "section"),
        P(("pb", "fsdp"), "section"),
        P("section", "fsdp"),
        P("fsdp", "pb", None),
        P(),
    )
    return jax.shard_map(
        shards, mesh=mesh, in_specs=placed, out_specs=P("pb", None, "fsdp"), check_vma=False
    )
```

```python
import jax
import jax.numpy as jnp
from jax import lax
from jax.experimental import pallas as pl
from jax.experimental.pallas import tpu as pltpu
from jax.sharding import PartitionSpec as P

HD = 64
BLOCK = 128
NEGATIVE = -1e30
MESH = pl.DeviceIdType.MESH
NZ = 8
NX = 4
NEAR = 512
FAR = 128
F32 = jnp.float32
BF16 = jnp.bfloat16


def kernel(
    mask_ref, ds_ref, gain_ref, qw_ref, kw_ref, vw_ref, ow_ref, pass_ref, out_ref,
    xs, ws, acc, ow, ds, gain, qw, qpart, qrecv, qsend, qbuf, part, recv, asend, att, osend, orecv,
    loc, pair_s, pair_r, y_s, y_r, ax_s, ax_r, az_s, az_r, bz_s, bz_r, bx_s, bx_r, cy_s, cy_r,
    q2_s, q2_r, q3_s, q3_r, ow_s, ow_r, t1_s, t1_r, t2_s, t2_r,
):
    s = lax.axis_index("section")
    p = lax.axis_index("pb")
    f = lax.axis_index("fsdp")
    z, c = p // 2, lax.rem(p, 2)
    x, y = f // 2, lax.rem(f, 2)

    def zat(k):
        return lax.rem(z + k + NZ, NZ)

    def xat(k):
        return lax.rem(x + k + NX, NX)

    def dev(s_, p_, f_):
        return {"section": s_, "pb": p_, "fsdp": f_}

    partner = dev(s, z * 2 + 1 - c, f)
    ynear = dev(s, p, x * 2 + 1 - y)
    xdev = {k: dev(s, p, xat(k) * 2 + y) for k in (1, -1)}
    zdev = {k: dev(s, zat(k) * 2 + c, f) for k in (1, -1)}
    other_section = dev(1 - s, p, f)

    def rcopy(src, dst, ssem, rsem, to):
        return pltpu.make_async_remote_copy(
            src_ref=src, dst_ref=dst, send_sem=ssem, recv_sem=rsem, device_id=to, device_id_type=MESH
        )

    def half(ref, h):
        return ref.at[:, pl.ds(pl.multiple_of(h * 512, 512), 512)]

    locals_ = [
        pltpu.make_async_copy(ds_ref, ds, loc.at[0]),
        pltpu.make_async_copy(gain_ref, gain, loc.at[1]),
        pltpu.make_async_copy(qw_ref, qw, loc.at[2]),
        pltpu.make_async_copy(half(kw_ref, c), ws.at[z, c, x, y, :, pl.ds(0, 512)], loc.at[3]),
        pltpu.make_async_copy(half(vw_ref, c), ws.at[z, c, x, y, :, pl.ds(512, 512)], loc.at[4]),
        pltpu.make_async_copy(pass_ref, xs.at[c], loc.at[5]),
        pltpu.make_async_copy(ow_ref, ow, loc.at[6]),
    ]
    for copy in locals_:
        copy.start()

    barrier = pltpu.get_barrier_semaphore()

    def greet(to):
        pl.semaphore_signal(barrier, inc=1, device_id=to, device_id_type=MESH)

    def q3_target(i):
        return plane(i), f // 4, z

    def t2_target(k):
        return f * 2 + z // 4, lax.rem(f + k, 8)

    diag = z == f
    for to in (partner, ynear, xdev[1], xdev[-1], zdev[1], zdev[-1], other_section):
        greet(to)
    pl.semaphore_wait(barrier, 7)

    sends = []

    def go(copy):
        copy.start()
        sends.append(copy)

    def pair_copy(i):
        w_ref = (kw_ref, vw_ref)[i]
        return rcopy(
            half(w_ref, 1 - c), ws.at[z, c, x, y, :, pl.ds(512 * i, 512)], pair_s.at[i], pair_r.at[i], partner
        )

    go(pair_copy(0))
    go(pair_copy(1))
    go(rcopy(pass_ref, xs.at[c], pair_s.at[2], pair_r.at[2], partner))

    def land(dst, rsem):
        rcopy(dst, dst, loc.at[7], rsem, partner).wait_recv()

    def plane(i):
        if i == 0:
            return z
        if i == NZ - 1:
            return zat(NZ // 2)
        return zat(-((i + 1) // 2)) if i % 2 else zat(i // 2)

    ys = (y, 1 - y)

    def piece_a(zz, xx, h):
        return ws.at[zz, :, xx, ys[h], :, pl.ds(0, (NEAR, FAR)[h])]

    def piece_b(zz, xx, h):
        return ws.at[zz, :, xx, ys[h], :, pl.ds(NEAR, 1024 - NEAR)]

    def piece_c(zz, h):
        return ws.at[zz, :, :, ys[h], :, pl.ds(FAR, NEAR - FAR)]

    def onward(i, parity):
        if i == NZ - 1:
            return None
        k = (i + 1) // 2
        way = 1 if i % 2 else -1
        if k + 1 < NZ // 2:
            return (i + 2, way)
        if (parity == 0) == (way == 1):
            return (NZ - 1, way)
        return None

    def z_sends(ref, i, col, ssem, rsem):
        nexts = [(1, 1), (2, -1)] if i == 0 else [onward(i, col % 2)]
        for step in nexts:
            if step is not None:
                slot, way = step
                go(rcopy(ref, ref, ssem.at[slot - 1, col], rsem.at[slot - 1, col], zdev[way]))

    xorder = (0, -1, 1, 2)

    def b_go(i, h):
        ref = piece_b(plane(i), x, h)
        for way in (1, -1):
            n = (1 - way) // 2
            go(rcopy(ref, ref, bx_s.at[i, h, n], bx_r.at[i, h, n], xdev[way]))
        z_sends(ref, i, h, bz_s, bz_r)

    def b_z(i):
        for h in range(2):
            land(piece_b(plane(i), x, h), bz_r.at[i - 1, h])
            b_go(i, h)

    def a_z(i):
        for j in range(4):
            for h in range(2):
                ref = piece_a(plane(i), xat(xorder[j]), h)
                land(ref, az_r.at[h, i - 1, j])
                z_sends(ref, i, j, az_s.at[h], az_r.at[h])

    def a_own(h):
        ref = piece_a(z, x, h)
        for way in (1, -1):
            n = (1 - way) // 2
            go(rcopy(ref, ref, ax_s.at[h, n], ax_r.at[h, n], xdev[way]))
        z_sends(ref, 0, 0, az_s.at[h], az_r.at[h])

    def a_x():
        for j in range(1, 4):
            for h in range(2):
                ref = piece_a(z, xat(xorder[j]), h)
                land(ref, ax_r.at[h, j - 1])
                if j == 1:
                    go(rcopy(ref, ref, ax_s.at[h, 2], ax_r.at[h, 2], xdev[1]))
                z_sends(ref, 0, j, az_s.at[h], az_r.at[h])

    def c_go(i):
        ref = piece_c(plane(i), 0)
        go(rcopy(ref, ref, cy_s.at[i], cy_r.at[i], ynear))

    def b_x1(i):
        for h in range(2):
            left, right = piece_b(plane(i), xat(-1), h), piece_b(plane(i), xat(1), h)
            land(left, bx_r.at[i, h, 0])
            land(right, bx_r.at[i, h, 1])
            ref, way = ((left, 1), (right, -1))[h]
            go(rcopy(ref, ref, bx_s.at[i, h, 2], bx_r.at[i, h, 2], xdev[way]))

    def last(i):
        for h in range(2):
            land(piece_b(plane(i), xat(2), h), bx_r.at[i, h, 2])
        land(piece_c(plane(i), 1), cy_r.at[i])

    def project(i):
        zz = plane(i)
        cols = pl.ds(pl.multiple_of(zz * 512, 512), 512)

        def tile(t, carry):
            rows = xs[t // 2, lax.rem(t, 2), :, cols]
            for n in range(4):
                w = ws[zz, :, :, :, :, n * 256 : (n + 1) * 256].reshape(512, 256)
                term = jnp.dot(rows, w, preferred_element_type=F32)
                at = (t, slice(None), slice(n * 256, (n + 1) * 256))
                if i == 0:
                    acc[at] = term
                else:
                    acc[at] += term
            return carry

        lax.fori_loop(0, 4, tile, 0)

    def query_start():
        for copy in locals_[:3]:
            copy.wait()
        wide = ds[...].astype(F32)
        squares = jnp.broadcast_to(jnp.sum(wide * wide, axis=1, keepdims=True), (32, 128))
        scaled = (wide * gain[...].astype(F32).reshape(1, 512)).astype(BF16)
        total = jnp.dot(scaled, qw[...], preferred_element_type=F32)
        for b in range(8):
            qpart[b, :, 0:128] = total[:, b * 128 : (b + 1) * 128]
            qpart[b, :, 128:256] = squares

    def query_reduce():
        for k in range(1, 8):
            to = lax.rem(f + k, 8)
            go(rcopy(qpart.at[to], qrecv.at[k - 1], q2_s.at[k - 1], q2_r.at[k - 1], dev(s, p, to)))

    def query_total():
        total = qpart[f]
        for k in range(7):
            land(qrecv.at[k], q2_r.at[k])
            total = total + qrecv[k]
        scale = lax.rsqrt(total[:, 128:256] / 4096.0 + 1e-06)
        qsend[...] = (total[:, 0:128] * scale).astype(BF16)

    def query_send(i):
        block = lax.rem(f, 4)
        zt, ct, ft = q3_target(i)
        copy = rcopy(qsend, qbuf.at[c, block], q3_s.at[i], q3_r.at[c * 4 + block], dev(s, zt * 2 + ct, ft))
        if i == 0:
            own = diag & (ct == c)

            @pl.when(own)
            def _():
                qbuf[c, block] = qsend[...]

            @pl.when(jnp.logical_not(own))
            def _():
                copy.start()

        else:
            go(copy)

    def query_wait():
        for cs in range(2):
            for b in range(4):
                own = diag & (f // 4 == c) & (cs == c) & (b == lax.rem(f, 4))

                @pl.when(jnp.logical_not(own))
                def _():
                    land(qbuf.at[cs, b], q3_r.at[cs * 4 + b])

        zt, ct, ft = q3_target(0)

        @pl.when(jnp.logical_not(diag & (ct == c)))
        def _():
            rcopy(qsend, qbuf.at[0, 0], q3_s.at[0], q3_r.at[0], partner).wait_send()

    def attend():
        head_of = lax.broadcasted_iota(jnp.int32, (32, 512), 1) // HD
        lane = lax.broadcasted_iota(jnp.int32, (32, 128), 1)
        block_of = lax.broadcasted_iota(jnp.int32, (256, 512), 1) // BLOCK
        for q in range(2):
            query = jnp.concatenate([qbuf[q, b] for b in range(4)], axis=1).astype(F32)
            spread = jnp.concatenate(
                [jnp.where(head_of == h, query, 0.0).astype(BF16) for h in range(8)], axis=0
            )
            keys = jnp.concatenate([acc[q, :, 0:512], acc[2 + q, :, 0:512]], axis=0).astype(BF16)
            values = jnp.concatenate([acc[q, :, 512:1024], acc[2 + q, :, 512:1024]], axis=0).astype(BF16)
            scores = lax.dot_general(spread, keys, (((1,), (1,)), ((), ())), preferred_element_type=F32)
            flags = jnp.zeros((256, 512), jnp.int32)
            for b in range(4):
                flags = jnp.where(block_of == b, mask_ref[f * 2 + q, z * 4 + b], flags)
            shown = flags > 0
            scores = jnp.where(shown, scores, NEGATIVE)
            peak = jnp.max(scores, axis=1, keepdims=True)
            raw = jnp.where(shown, jnp.exp(scores - peak), 0.0)
            totals = jnp.sum(raw, axis=1, keepdims=True)
            wide = jnp.dot(raw.astype(BF16), values, preferred_element_type=F32)
            numer = jnp.zeros((32, 512), F32)
            stats = jnp.zeros((32, 128), F32)
            for h in range(8):
                rows = slice(h * 32, (h + 1) * 32)
                numer = jnp.where(head_of == h, wide[rows], numer)
                stats = jnp.where(lane == h, peak[rows], stats)
                stats = jnp.where(lane == h + 64, totals[rows], stats)
            for ah in range(2):
                rows = slice(ah * 16, (ah + 1) * 16)
                for ch in range(2):
                    rank = (q * 2 + ah) * 2 + ch
                    part[rank, :, 0:256] = numer[rows, ch * 256 : (ch + 1) * 256]
                    part[rank, :, 256:384] = stats[rows]

    def combine_send():
        for k in range(1, 8):
            zt = zat(k)
            go(rcopy(part.at[zt], recv.at[k - 1], t1_s.at[k - 1], t1_r.at[k - 1], dev(s, zt * 2 + c, f)))

    def combine():
        pieces = [part[z]]
        for k in range(7):
            land(recv.at[k], t1_r.at[k])
            pieces.append(recv[k])
        top = pieces[0][:, 256:384]
        for piece in pieces[1:]:
            top = jnp.maximum(top, piece[:, 256:384])
        col_head = lax.broadcasted_iota(jnp.int32, (16, 256), 1) // HD
        first = lax.rem(z, 2) == 0

        def widen(stat, base):
            low = jnp.zeros((16, 256), F32)
            for h in range(4):
                one = jnp.where(first, stat[:, base + h : base + h + 1], stat[:, base + h + 4 : base + h + 5])
                low = jnp.where(col_head == h, one, low)
            return low

        top_wide = widen(top, 0)
        numer = jnp.zeros((16, 256), F32)
        total = jnp.zeros((16, 256), F32)
        for piece in pieces:
            stat = piece[:, 256:384]
            factor = jnp.exp(widen(stat, 0) - top_wide)
            numer = numer + piece[:, 0:256] * factor
            total = total + widen(stat, 64) * factor
        asend[...] = (numer / total).astype(BF16)

    def spot():
        return c, lax.rem(z, 2), lax.rem(z // 2, 2)

    def scatter():
        b, d, e = spot()
        sem = t2_r.at[(b * 2 + d) * 2 + e]
        for k in range(8):
            pt, ft = t2_target(k)
            copy = rcopy(asend, att.at[b, d, e], t2_s.at[k], sem, dev(s, pt, ft))
            if k == 0:
                own = pt == p

                @pl.when(own)
                def _():
                    att[b, d, e] = asend[...]

                @pl.when(jnp.logical_not(own))
                def _():
                    copy.start()

            else:
                go(copy)

    def finish():
        locals_[6].wait()
        b, d, e = spot()
        own_code = (b * 2 + d) * 2 + e
        pt, ft = t2_target(0)
        own = pt == p
        total = jnp.zeros((32, 512), F32)
        for ci in range(2):
            for ch in range(2):
                halves = []
                for ah in range(2):
                    code = (ci * 2 + ch) * 2 + ah

                    @pl.when(jnp.logical_not(own & (own_code == code)))
                    def _():
                        land(att.at[ci, ch, ah], t2_r.at[code])

                    halves.append(att[ci, ch, ah])
                rows = jnp.concatenate(halves, axis=0)
                at = ci * 512 + ch * 256
                total = total + jnp.dot(rows, ow[at : at + 256, :], preferred_element_type=F32)
        osend[...] = total.astype(BF16)
        go(rcopy(osend, orecv, ow_s.at[0], ow_r.at[0], other_section))
        land(orecv, ow_r.at[0])
        out_ref[...] = (osend[...].astype(F32) + orecv[...].astype(F32)).astype(BF16)

        @pl.when(jnp.logical_not(own))
        def _():
            rcopy(asend, att.at[0, 0, 0], t2_s.at[0], t2_r.at[0], partner).wait_send()

    locals_[3].wait()
    locals_[4].wait()
    land(ws.at[z, 1 - c, x, y, :, pl.ds(0, 512)], pair_r.at[0])
    land(ws.at[z, 1 - c, x, y, :, pl.ds(512, 512)], pair_r.at[1])
    own_b, own_c = piece_b(z, x, 0), ws.at[z, :, x, y, :, pl.ds(0, FAR)]
    go(rcopy(own_b, own_b, y_s.at[0], y_r.at[0], ynear))
    go(rcopy(own_c, own_c, y_s.at[1], y_r.at[1], ynear))
    b_go(0, 0)
    a_own(0)
    query_start()
    land(piece_b(z, x, 1), y_r.at[0])
    b_go(0, 1)
    land(piece_a(z, x, 1), y_r.at[1])
    a_own(1)
    a_x()
    c_go(0)
    query_reduce()
    for t in range(1, NZ + 2):
        if t < NZ:
            b_z(t)
            a_z(t)
            c_go(t)
        if t <= NZ:
            b_x1(t - 1)
        if t == 2:
            query_total()
            query_send(0)
            query_send(1)
            locals_[5].wait()
            land(xs.at[1 - c], pair_r.at[2])
        if 2 <= t < NZ:
            query_send(t)
        if t >= 2:
            last(t - 2)
            project(t - 2)
    query_wait()
    attend()
    combine_send()
    combine()
    scatter()
    finish()
    for copy in sends:
        copy.wait_send()


def shards(
    decoder_states, norm_gain, query_weight, key_weight, value_weight, out_weight, passage_states, block_mask
):
    anywhere = pl.BlockSpec(memory_space=pl.ANY)
    dma = pltpu.SemaphoreType.DMA
    out = pl.pallas_call(
        kernel,
        out_shape=jax.ShapeDtypeStruct((32, 512), BF16),
        in_specs=[pl.BlockSpec(memory_space=pltpu.SMEM)] + [anywhere] * 7,
        out_specs=pl.BlockSpec(memory_space=pltpu.VMEM),
        scratch_shapes=[
            pltpu.VMEM((2, 2, 256, 4096), BF16),
            pltpu.VMEM((NZ, 2, NX, 2, 32, 1024), BF16),
            pltpu.VMEM((4, 256, 1024), F32),
            pltpu.VMEM((1024, 512), BF16),
            pltpu.VMEM((32, 512), BF16),
            pltpu.VMEM((512,), BF16),
            pltpu.VMEM((512, 1024), BF16),
            pltpu.VMEM((8, 32, 256), F32),
            pltpu.VMEM((7, 32, 256), F32),
            pltpu.VMEM((32, 128), BF16),
            pltpu.VMEM((2, 4, 32, 128), BF16),
            pltpu.VMEM((8, 16, 384), F32),
            pltpu.VMEM((7, 16, 384), F32),
            pltpu.VMEM((16, 256), BF16),
            pltpu.VMEM((2, 2, 2, 16, 256), BF16),
            pltpu.VMEM((32, 512), BF16),
            pltpu.VMEM((32, 512), BF16),
            dma((8,)),
            dma((3,)), dma((3,)),
            dma((2,)), dma((2,)),
            dma((2, 3)), dma((2, 3)),
            dma((2, NZ - 1, 4)), dma((2, NZ - 1, 4)),
            dma((NZ - 1, 2)), dma((NZ - 1, 2)),
            dma((NZ, 2, 3)), dma((NZ, 2, 3)),
            dma((NZ,)), dma((NZ,)),
            dma((7,)), dma((7,)),
            dma((8,)), dma((8,)),
            dma((1,)), dma((1,)),
            dma((7,)), dma((7,)),
            dma((8,)), dma((8,)),
        ],
        compiler_params=pltpu.CompilerParams(
            collective_id=0, has_side_effects=True, vmem_limit_bytes=56 * 1024 * 1024
        ),
        name="reader",
    )(
        block_mask, decoder_states[0], norm_gain, query_weight, key_weight, value_weight,
        out_weight, passage_states,
    )
    return out[None]


def solution(mesh):
    placed = (
        P("pb", None, "fsdp"),
        P("fsdp"),
        P("fsdp", "section"),
        P(("pb", "fsdp"), "section"),
        P(("pb", "fsdp"), "section"),
        P("section", "fsdp"),
        P("fsdp", "pb", None),
        P(),
    )
    return jax.shard_map(
        shards, mesh=mesh, in_specs=placed, out_specs=P("pb", None, "fsdp"), check_vma=False
    )
```
